32 devices in a mesh: band: 4 (over y, x), chan: 8 (over z, core).
Axes of the slice: x: 2, y: 2, z: 4, core: 2. Of those that a mesh axis runs over, the one named last changes fastest.
Arguments:
- coeffs: bfloat16 [2, 8, 1024, 4096], P(None, None, 'chan', 'band'), may hold values from -1100 to 1100, as said below
Outputs:
- coherence: float32 [1024, 1024], P('chan', 'band')
The draws below stay inside these ranges and needn't reach their ends.
Inputs may be any that keep to these rules, and one draw needn't show every extreme that they name: `coeffs`: finite real and imaginary parts.
All inputs are finite; a program needn't handle non-finite values.
Results may differ from the reference program's by a relative error of at most 0.0003.
Values may be sent and summed in bfloat16 or wider, within the bound.
A program may use at most 192 MiB of HBM per device.

```python
import jax
import jax.numpy as jnp
from jax import lax

C = 1024
K = 8
W = 16
BINS = 4096


def draw_coeffs(key, part):
    noise_key = jax.random.fold_in(jax.random.fold_in(key, 17), 0)
    noise = jnp.clip(jax.random.normal(noise_key, (2, K, C, BINS), jnp.float32), -6.0, 6.0)
    values = noise
    return values.astype(jnp.bfloat16)


def setup_inputs(seed: int = 0) -> dict:
    splits = jax.random.split(jax.random.key(seed), 2)
    return {
        "coeffs": draw_coeffs(jax.random.fold_in(splits[1], 71), 0),
    }


epsilon = 1e-6


def band_term(total, block):
    width = block.shape[2]
    flat = block.transpose(2, 0, 1, 3).reshape(width, -1)
    paired = jnp.stack((block[1], -block[0]), axis=0).transpose(2, 0, 1, 3).reshape(width, -1)
    real_part = jnp.dot(flat, flat.T, preferred_element_type=jnp.float32)
    imag_part = jnp.dot(paired, flat.T, preferred_element_type=jnp.float32)
    wide = flat.astype(jnp.float32)
    power = jnp.sum(wide * wide, axis=1) + epsilon
    coh_band = (real_part * real_part + imag_part * imag_part) / (power[:, None] * power[None, :])
    return total + coh_band, None


def reference(coeffs):
    num_bands = BINS // W
    width = coeffs.shape[2]
    blocks = coeffs.reshape(2, K, width, num_bands, W)
    blocks = jnp.moveaxis(blocks, 3, 0)
    total, unused = lax.scan(band_term, jnp.zeros((width, width), jnp.float32), blocks)
    rows = lax.broadcasted_iota(jnp.int32, (width, width), 0)
    cols = lax.broadcasted_iota(jnp.int32, (width, width), 1)
    total = jnp.where(rows == cols, jnp.float32(0.0), total)
    return total * jnp.float32(W * K / num_bands)
```

```python
import jax
import jax.numpy as jnp
from jax import lax
from jax.experimental import pallas as pl
from jax.experimental.pallas import tpu as pltpu
from jax.sharding import PartitionSpec as P

W = 16
LANE = 128

epsilon = 1e-06

MESH = pl.DeviceIdType.MESH


def quarter(side, z):
    seen = z + side * (3 - 2 * z)
    far = seen // 2
    return far * seen + (1 - far) * (1 - seen)


def group(side, q):
    far = q // 2
    seen = far * q + (1 - far) * (1 - q)
    return seen + side * (3 - 2 * seen)


def kernel(
    scale,
    x_ref,
    out_ref,
    buf,
    sel,
    xb,
    xq,
    inv_col,
    inv_row,
    part,
    land,
    zsend,
    zland,
    fin,
    fland,
    coef_send,
    coef_recv,
    part_send,
    part_recv,
    z_send,
    z_recv,
    fin_send,
    fin_recv,
):
    n = lax.axis_size("chan")
    groups = lax.axis_size("band")
    me = lax.axis_index("chan")
    column = lax.axis_index("band")
    strips, parts, tapers, strip, lanes = buf.shape
    bands, full, depth = xb.shape
    half = depth // 2
    m = n // 4
    own = full // n
    splits = strips // 4
    rows = own // splits
    quad = strips // 2
    shares = groups // 4
    members = groups * m
    per = LANE // W

    z = lax.div(me, m)
    lane = lax.rem(me, m)
    side = lax.div(z, 2)
    is_hub = (z == 1) | (z == 2)
    member = lane * groups + column

    barrier = pltpu.get_barrier_semaphore()
    for g in range(groups):
        for c in range(n):
            if g or c:
                pl.semaphore_signal(
                    barrier,
                    inc=1,
                    device_id={"band": lax.rem(column + g, groups), "chan": lax.rem(me + c, n)},
                    device_id_type=MESH,
                )
    pl.semaphore_wait(barrier, n * groups - 1)

    def coef_copy(far, s, t):
        to_side = side + far * (1 - 2 * side)
        hub = m + to_side * m + t
        w = quarter(to_side, z) * splits + s
        src = x_ref.at[
            :, :, pl.ds(s * rows, rows), pl.ds(pl.multiple_of((hub - m) * lanes, LANE), lanes)
        ]
        dst = buf.at[w, :, :, pl.ds(pl.multiple_of(lane * rows, rows), rows), :]
        recv = coef_recv.at[w, lane]

        def remote():
            return pltpu.make_async_remote_copy(
                src_ref=src,
                dst_ref=dst,
                send_sem=coef_send.at[far, s, t],
                recv_sem=recv,
                device_id={"chan": hub},
                device_id_type=MESH,
            )

        return hub, remote, lambda: pltpu.make_async_copy(src, dst, recv)

    for far in range(2):
        for s in range(splits):
            for t in range(m):
                hub, remote, local = coef_copy(far, s, t)
                if far:
                    remote().start()
                else:
                    pl.when(hub != me)(lambda: remote().start())
                    pl.when(hub == me)(lambda: local().start())

    def reducer(w, c):
        cross = lax.div(w, quad) * (1 - lax.div(c, quad))
        return lax.rem(lax.rem(w, quad) + lax.rem(c, quad), quad) + quad * cross

    def part_copy(w, c, to):
        rel = lax.rem(member - to + members, members)
        return pltpu.make_async_remote_copy(
            src_ref=part.at[w, c],
            dst_ref=land.at[w, rel],
            send_sem=part_send.at[w, c],
            recv_sem=part_recv.at[w, rel],
            device_id={
                "band": lax.rem(to, groups),
                "chan": m + side * m + lax.div(to, groups),
            },
            device_id_type=MESH,
        )

    def role(w):
        turn = lax.rem(member, quad)
        cross = lax.div(member, quad)
        upper = lax.div(w, quad)
        place = lax.rem(w, quad)
        q = lax.rem(turn - place + quad, quad)
        c = q + quad * upper * (1 - cross)
        valid = ((cross == 0) & (q <= place)) | ((cross == 1) & (upper == 1))
        other = jnp.where(cross == 1, q + quad, w + quad)
        crossing = cross == 1
        sends = valid & (
            (~crossing & (upper == 0))
            | (crossing & ((w < other) | ((w == other) & (side == 1))))
        )
        keeps = valid & (
            (~crossing & (upper == 1))
            | (crossing & ((w > other) | ((w == other) & (side == 0))))
        )
        return c, other, crossing, valid, sends, keeps

    def z_copy(w, other):
        return pltpu.make_async_remote_copy(
            src_ref=zsend.at[w],
            dst_ref=zland.at[other],
            send_sem=z_send.at[w],
            recv_sem=z_recv.at[other],
            device_id={"chan": m + (1 - side) * m + lane},
            device_id_type=MESH,
        )

    def final_copies(w, c):
        for turned in range(2):
            row, col = (c, w) if turned else (w, c)
            zr, zc = group(side, lax.div(row, splits)), group(side, lax.div(col, splits))
            sr, sc = lax.rem(row, splits), lax.rem(col, splits)
            for t in range(m):
                for j in range(shares):
                    chan, band = zr * m + t, zc * shares + j
                    src = fin.at[w, turned, pl.ds(t * rows, rows), :]
                    dst = fland.at[sr, sc]

                    def remote():
                        return pltpu.make_async_remote_copy(
                            src_ref=src,
                            dst_ref=dst,
                            send_sem=fin_send.at[w, turned, t, j],
                            recv_sem=fin_recv.at[sr, sc],
                            device_id={"band": band, "chan": chan},
                            device_id_type=MESH,
                        )

                    def local():
                        return pltpu.make_async_copy(src, dst, fin_recv.at[sr, sc])

                    mine = (chan == me) & (band == column)
                    wanted = (w != c) if turned else True
                    yield wanted, mine, remote, local

    def relayout(w):
        rows_w = pl.ds(pl.multiple_of(w * strip, strip), strip)
        at = lax.broadcasted_iota(jnp.int32, (strip, LANE), 1)
        power = jnp.ones((strip, LANE), jnp.float32)
        for v in range(lanes // LANE):
            window = slice(v * LANE, (v + 1) * LANE)
            both = jnp.concatenate(
                [
                    jnp.concatenate([buf[w, p, k, :, window] for k in range(tapers)], axis=1)
                    for p in range(parts)
                ],
                axis=0,
            )
            for d in range(per // 2):
                chosen = sel[:, 2 * d * half : 2 * (d + 1) * half]
                picked = jnp.dot(both, chosen, preferred_element_type=jnp.float32)
                for e in range(2):
                    b = v * per + 2 * d + e
                    re = picked[:strip, e * half : (e + 1) * half]
                    im = picked[strip:, e * half : (e + 1) * half]
                    total = jnp.sum(re * re + im * im, axis=1, keepdims=True) + epsilon
                    power = jnp.where(at == b, total, power)
                    xb[b, rows_w, :half] = re.astype(jnp.bfloat16)
                    xb[b, rows_w, half:] = im.astype(jnp.bfloat16)
                    xq[b, :, :half] = im.astype(jnp.bfloat16)
                    xq[b, :, half:] = (-re).astype(jnp.bfloat16)
        inverse = 1.0 / power
        inv_col[...] = inverse
        inv_row[:, pl.ds(pl.multiple_of(w * strip, strip), strip)] = inverse.T[:bands, :]

    contract = (((1,), (1,)), ((), ()))

    def gram(w):
        rows_w = pl.ds(pl.multiple_of(w * strip, strip), strip)

        def pair(v, carry):
            cols = pl.ds(pl.multiple_of(v * 2 * strip, 2 * strip), 2 * strip)
            acc = jnp.zeros((strip, 2 * strip), jnp.float32)
            for b in range(bands):
                left = jnp.concatenate([xb[b, rows_w, :], xq[b]], axis=0)
                both = lax.dot_general(
                    left, xb[b, cols, :], contract, preferred_element_type=jnp.float32
                )
                re, im = both[:strip], both[strip:]
                acc += ((re * re + im * im) * inv_col[:, b : b + 1]) * inv_row[b : b + 1, cols]
            for e in range(2):
                part[w, 2 * v + e] = acc[:, e * strip : (e + 1) * strip]
            for e in range(2):
                c = 2 * v + e
                to = reducer(w, c)

                @pl.when((c <= w) & (to != member))
                def _():
                    part_copy(w, c, to).start()

            return carry

        lax.fori_loop(0, lax.div(w, 2) + 1, pair, 0)

    def reduce(w):
        c, other, crossing, valid, sends, keeps = role(w)

        @pl.when(valid)
        def _():
            for rel in range(1, members):
                pltpu.make_async_copy(land.at[w, rel], land.at[w, rel], part_recv.at[w, rel]).wait()
            total = part[w, c]
            for rel in range(1, members):
                total += land[w, rel]

            @pl.when(sends & crossing)
            def _():
                zsend[w] = total.T

            @pl.when(sends & ~crossing)
            def _():
                zsend[w] = total

            @pl.when(sends)
            def _():
                z_copy(w, other).start()

            @pl.when(keeps)
            def _():
                pltpu.make_async_copy(zland.at[w], zland.at[w], z_recv.at[w]).wait()
                whole = total + zland[w]
                fin[w, 0] = whole
                fin[w, 1] = whole.T
                for wanted, mine, remote, local in final_copies(w, c):
                    pl.when(wanted & ~mine)(lambda: remote().start())
                    pl.when(wanted & mine)(lambda: local().start())

    @pl.when(is_hub)
    def _():
        row = lax.broadcasted_iota(jnp.int32, (LANE, per * half), 0)
        col = lax.broadcasted_iota(jnp.int32, (LANE, per * half), 1)
        band, within = col // half, col % half
        for k in range(tapers):
            hit = (row == band * W + within - k * W) & (within // W == k)
            sel[k * LANE : (k + 1) * LANE, :] = jnp.where(hit, 1.0, 0.0).astype(jnp.bfloat16)

        def step(w, carry):
            for t in range(m):
                dst = buf.at[w, :, :, pl.ds(t * rows, rows), :]
                pltpu.make_async_copy(dst, dst, coef_recv.at[w, t]).wait()
            relayout(w)
            gram(w)
            pl.when(w > 0)(lambda: reduce(w - 1))
            return carry

        lax.fori_loop(0, strips, step, 0)
        reduce(strips - 1)

        def drain(w, carry):
            def tile(c, carry):
                to = reducer(w, c)
                pl.when(to != member)(lambda: part_copy(w, c, to).wait_send())
                return carry

            lax.fori_loop(0, w + 1, tile, 0)
            c, other, crossing, valid, sends, keeps = role(w)
            pl.when(sends)(lambda: z_copy(w, other).wait_send())

            @pl.when(keeps)
            def _():
                for wanted, mine, remote, local in final_copies(w, c):
                    pl.when(wanted & ~mine)(lambda: remote().wait_send())

            return carry

        lax.fori_loop(0, strips, drain, 0)

    for far in range(2):
        for s in range(splits):
            for t in range(m):
                hub, remote, local = coef_copy(far, s, t)
                if far:
                    remote().wait_send()
                else:
                    pl.when(hub != me)(lambda: remote().wait_send())

    width = out_ref.shape[1]
    here = lax.rem(column, shares)
    per_share = m // shares
    for s in range(splits):
        for sc in range(splits):
            pltpu.make_async_copy(fland.at[s, sc], fland.at[s, sc], fin_recv.at[s, sc]).wait()
        choice = None
        for j in range(shares):
            pieces = [
                fland[s, sc, :, t * rows : (t + 1) * rows]
                for t in range(j * per_share, (j + 1) * per_share)
                for sc in range(splits)
            ]
            value = jnp.concatenate(pieces, axis=1)
            choice = value if choice is None else jnp.where(here == j, value, choice)
        row = lax.broadcasted_iota(jnp.int32, (rows, width), 0) + (me * own + s * rows)
        col = lax.broadcasted_iota(jnp.int32, (rows, width), 1) + column * width
        out_ref[s * rows : (s + 1) * rows, :] = jnp.where(row == col, 0.0, choice) * scale


def body(coeffs):
    parts, tapers, own, bins = coeffs.shape
    n = lax.axis_size("chan")
    groups = lax.axis_size("band")
    full = own * n
    m = n // 4
    hubs = 2 * m
    lanes = bins // hubs
    bands = lanes // W
    depth = parts * tapers * W
    strip = LANE
    strips = full // strip
    splits = strips // 4
    rows = own // splits
    members = groups * m
    shares = groups // 4
    scale = W * tapers / (bins // W * groups)
    dma = pltpu.SemaphoreType.DMA

    def run(*refs):
        kernel(scale, *refs)

    return pl.pallas_call(
        run,
        out_shape=jax.ShapeDtypeStruct((own, full // groups), jnp.float32),
        in_specs=[pl.BlockSpec(memory_space=pl.ANY)],
        out_specs=pl.BlockSpec(memory_space=pltpu.VMEM),
        scratch_shapes=[
            pltpu.VMEM((strips, parts, tapers, strip, lanes), jnp.bfloat16),
            pltpu.VMEM((tapers * LANE, LANE // W * depth // 2), jnp.bfloat16),
            pltpu.VMEM((bands, full, depth), jnp.bfloat16),
            pltpu.VMEM((bands, strip, depth), jnp.bfloat16),
            pltpu.VMEM((strip, LANE), jnp.float32),
            pltpu.VMEM((bands, full), jnp.float32),
            pltpu.VMEM((strips, strips, strip, strip), jnp.float32),
            pltpu.VMEM((strips, members, strip, strip), jnp.float32),
            pltpu.VMEM((strips, strip, strip), jnp.float32),
            pltpu.VMEM((strips, strip, strip), jnp.float32),
            pltpu.VMEM((strips, 2, strip, strip), jnp.float32),
            pltpu.VMEM((splits, splits, rows, strip), jnp.float32),
            dma((2, splits, m)),
            dma((strips, m)),
            dma((strips, strips)),
            dma((strips, members)),
            dma((strips,)),
            dma((strips,)),
            dma((strips, 2, m, shares)),
            dma((splits, splits)),
        ],
        compiler_params=pltpu.CompilerParams(
            collective_id=0, has_side_effects=True, vmem_limit_bytes=56 * 1024 * 1024
        ),
    )(coeffs)


def solution(mesh):
    return jax.shard_map(
        body,
        mesh=mesh,
        in_specs=(P(None, None, "chan", "band"),),
        out_specs=P("chan", "band"),
        check_vma=False,
    )
```

```python
import jax
import jax.numpy as jnp
from jax import lax
from jax.experimental import pallas as pl
from jax.experimental.pallas import tpu as pltpu
from jax.sharding import PartitionSpec as P

W = 16
LANE = 128
SUBS = 2

epsilon = 1e-06

MESH = pl.DeviceIdType.MESH


def quarter(side, z):
    seen = z + side * (3 - 2 * z)
    far = seen // 2
    return far * seen + (1 - far) * (1 - seen)


def group(side, q):
    far = q // 2
    seen = far * q + (1 - far) * (1 - q)
    return seen + side * (3 - 2 * seen)


def kernel(
    scale,
    x_ref,
    out_ref,
    buf,
    sel,
    xb,
    xq,
    inv_col,
    inv_row,
    part,
    land,
    total,
    zsend,
    zland,
    fin,
    fland,
    coef_send,
    coef_recv,
    part_send,
    part_recv,
    z_send,
    z_recv,
    fin_send,
    fin_recv,
    ready,
    met,
    go,
):
    n = lax.axis_size("chan")
    groups = lax.axis_size("band")
    me = lax.axis_index("chan")
    column = lax.axis_index("band")
    strips, parts, tapers, strip, lanes = buf.shape
    splits, subs, rows = fland.shape[1:4]
    bands, full, depth = xb.shape
    half = depth // 2
    m = n // 4
    own = full // n
    quad = strips // 2
    shares = groups // 4
    members = groups * m
    per = LANE // W
    slab = strip // subs

    z = lax.div(me, m)
    lane = lax.rem(me, m)
    side = lax.div(z, 2)
    is_hub = (z == 1) | (z == 2)
    member = lane * groups + column
    mine = quarter(side, lax.div(column, shares)) * splits + lane
    reduces = (lane < splits) & (lax.rem(column, shares) == 0)

    barrier = pltpu.get_barrier_semaphore()
    envoy = m + 1
    is_envoy = me == envoy

    @pl.when(is_hub)
    def _():
        for c in range(1, n):
            pl.semaphore_signal(
                barrier, inc=1, device_id={"chan": lax.rem(me + c, n)}, device_id_type=MESH
            )

    @pl.when(is_envoy)
    def _():
        for g in range(1, groups):
            pl.semaphore_signal(
                barrier,
                inc=1,
                device_id={"band": lax.rem(column + g, groups)},
                device_id_type=MESH,
            )

    pl.semaphore_wait(
        barrier, 2 * m - is_hub.astype(jnp.int32) + is_envoy.astype(jnp.int32) * (groups - 1)
    )

    def coef_copy(far, s, i, t):
        to_side = side + far * (1 - 2 * side)
        hub = m + to_side * m + t
        w = quarter(to_side, z) * splits + s
        src = x_ref.at[
            :,
            :,
            pl.ds((s * subs + i) * rows, rows),
            pl.ds(pl.multiple_of((hub - m) * lanes, LANE), lanes),
        ]
        dst = buf.at[w, :, :, pl.ds(pl.multiple_of(i * slab + lane * rows, rows), rows), :]
        recv = coef_recv.at[w, i, lane]

        def remote():
            return pltpu.make_async_remote_copy(
                src_ref=src,
                dst_ref=dst,
                send_sem=coef_send.at[far, s, i, t],
                recv_sem=recv,
                device_id={"chan": hub},
                device_id_type=MESH,
            )

        return hub, remote, lambda: pltpu.make_async_copy(src, dst, recv)

    order = [
        (far, s, i, t) for far in range(2) for s in range(splits) for i in range(subs) for t in range(m)
    ]
    for far, s, i, t in order:
        hub, remote, local = coef_copy(far, s, i, t)
        if far:
            remote().start()
        else:
            pl.when(hub != me)(lambda: remote().start())
            pl.when(hub == me)(lambda: local().start())

    @pl.when(~is_hub)
    def _():
        pl.semaphore_signal(ready, inc=1, device_id={"chan": envoy}, device_id_type=MESH)

    def meet():
        @pl.when(is_envoy)
        def _():
            pl.semaphore_wait(ready, n - 2 * m)
            for g in range(1, groups):
                pl.semaphore_signal(
                    met,
                    inc=1,
                    device_id={"band": lax.rem(column + g, groups)},
                    device_id_type=MESH,
                )
            pl.semaphore_wait(met, groups - 1)
            for h in range(2 * m):
                if m + h != envoy:
                    pl.semaphore_signal(go, inc=1, device_id={"chan": m + h}, device_id_type=MESH)

        @pl.when(~is_envoy)
        def _():
            pl.semaphore_wait(go, 1)

    def place(to_side, c):
        band = group(to_side, lax.div(c, splits)) * shares
        at = lax.rem(c, splits)
        return band, m + to_side * m + at, at * groups + band

    def part_copy(w, c):
        band, chan, to = place(side, c)
        return pltpu.make_async_remote_copy(
            src_ref=part.at[w, c],
            dst_ref=land.at[w, lax.rem(member - to + members, members)],
            send_sem=part_send.at[w, c],
            recv_sem=part_recv.at[w],
            device_id={"band": band, "chan": chan},
            device_id_type=MESH,
        )

    def role(w):
        c = mine
        valid = reduces & (c <= w)
        upper = w >= quad
        crossing = upper & (c < quad)
        even = w == c + quad
        sends = valid & (
            (w < quad) | (crossing & ((w < c + quad) | (even & (side == 1))))
        )
        keeps = valid & (
            (c >= quad) | (crossing & ((w > c + quad) | (even & (side == 0))))
        )
        return crossing, valid, sends, keeps

    def z_copy(w):
        crossed = lax.div(w, quad)
        to = crossed * (w - quad) + (1 - crossed) * (mine + quad)
        slot = crossed * (mine + quad) + (1 - crossed) * (w + quad)
        band, chan, unused = place(1 - side, to)
        return pltpu.make_async_remote_copy(
            src_ref=zsend.at[w],
            dst_ref=zland.at[slot],
            send_sem=z_send.at[w],
            recv_sem=z_recv.at[slot],
            device_id={"band": band, "chan": chan},
            device_id_type=MESH,
        )

    def final_copies(w):
        for turned in range(2):
            row, col = (mine, w) if turned else (w, mine)
            zr, zc = group(side, lax.div(row, splits)), group(side, lax.div(col, splits))
            sr, sc = lax.rem(row, splits), lax.rem(col, splits)
            for t in range(m):
                for j in range(shares):
                    chan, band = zr * m + t, zc * shares + j
                    src = fin.at[w, turned, :, t]
                    dst = fland.at[sr, sc]

                    def remote():
                        return pltpu.make_async_remote_copy(
                            src_ref=src,
                            dst_ref=dst,
                            send_sem=fin_send.at[w, turned, t, j],
                            recv_sem=fin_recv.at[sr, sc],
                            device_id={"band": band, "chan": chan},
                            device_id_type=MESH,
                        )

                    def local():
                        return pltpu.make_async_copy(src, dst, fin_recv.at[sr, sc])

                    here = (chan == me) & (band == column)
                    wanted = (w != mine) if turned else True
                    yield wanted, here, remote, local

    def relayout(w, i):
        rows_w = pl.ds(pl.multiple_of(w * strip + i * slab, slab), slab)
        at = lax.broadcasted_iota(jnp.int32, (slab, LANE), 1)
        power = jnp.ones((slab, LANE), jnp.float32)
        inside = pl.ds(pl.multiple_of(i * slab, slab), slab)
        for v in range(lanes // LANE):
            window = slice(v * LANE, (v + 1) * LANE)
            both = jnp.concatenate(
                [
                    jnp.concatenate([buf[w, p, k, inside, window] for k in range(tapers)], axis=1)
                    for p in range(parts)
                ],
                axis=0,
            )
            for d in range(per // 2):
                chosen = sel[:, 2 * d * half : 2 * (d + 1) * half]
                picked = jnp.dot(both, chosen, preferred_element_type=jnp.float32)
                for e in range(2):
                    b = v * per + 2 * d + e
                    re = picked[:slab, e * half : (e + 1) * half]
                    im = picked[slab:, e * half : (e + 1) * half]
                    sums = jnp.sum(re * re + im * im, axis=1, keepdims=True) + epsilon
                    power = jnp.where(at == b, sums, power)
                    xb[b, rows_w, :half] = re.astype(jnp.bfloat16)
                    xb[b, rows_w, half:] = im.astype(jnp.bfloat16)
                    xq[b, inside, :half] = im.astype(jnp.bfloat16)
                    xq[b, inside, half:] = (-re).astype(jnp.bfloat16)
        inv_col[inside, :] = 1.0 / power
        inv_row[:, pl.ds(pl.multiple_of(w * strip, strip), strip)] = inv_col[...].T[:bands, :]

    contract = (((1,), (1,)), ((), ()))

    def gram(w):
        rows_w = pl.ds(pl.multiple_of(w * strip, strip), strip)
        at = lax.div(column, shares)

        def pair(k, carry):
            pl.when((w == strips - 1) & (k == 3))(finish_early)
            seat = jnp.where(
                k == 0,
                3 - at,
                jnp.where(k == 1, lax.rem(at + 2, 4), jnp.where(k == 2, at + 1 - 2 * lax.rem(at, 2), at)),
            )
            v = quarter(side, seat)

            @pl.when(2 * v <= w)
            def _():
                cols = pl.ds(pl.multiple_of(v * 2 * strip, 2 * strip), 2 * strip)
                acc = jnp.zeros((strip, 2 * strip), jnp.float32)
                for b in range(bands):
                    left = jnp.concatenate([xb[b, rows_w, :], xq[b]], axis=0)
                    both = lax.dot_general(
                        left, xb[b, cols, :], contract, preferred_element_type=jnp.float32
                    )
                    re, im = both[:strip], both[strip:]
                    acc += ((re * re + im * im) * inv_col[:, b : b + 1]) * inv_row[b : b + 1, cols]
                for e in range(2):
                    part[w, 2 * v + e] = acc[:, e * strip : (e + 1) * strip]
                for e in range(2):
                    c = 2 * v + e
                    to = place(side, c)[2]
                    pl.when((c <= w) & (to != member))(lambda: part_copy(w, c).start())

            return carry

        lax.fori_loop(0, 4, pair, 0)

    def reduce(w):
        crossing, valid, sends, keeps = role(w)

        @pl.when(valid)
        def _():
            every = land.at[w, pl.ds(1, members - 1)]
            pltpu.make_async_copy(every, every, part_recv.at[w]).wait()
            summed = part[w, mine]
            for rel in range(1, members):
                summed += land[w, rel]

            @pl.when(sends & crossing)
            def _():
                zsend[w] = summed.T

            @pl.when(sends & ~crossing)
            def _():
                zsend[w] = summed

            @pl.when(sends)
            def _():
                z_copy(w).start()

            @pl.when(keeps)
            def _():
                total[w] = summed

    def finish(w):
        crossing, valid, sends, keeps = role(w)

        @pl.when(keeps)
        def _():
            pltpu.make_async_copy(zland.at[w], zland.at[w], z_recv.at[w]).wait()
            whole = total[w] + zland[w]
            turned = whole.T
            fin[w, 0] = whole.reshape(subs, m, rows, strip)
            fin[w, 1] = turned.reshape(subs, m, rows, strip)
            for wanted, here, remote, local in final_copies(w):
                pl.when(wanted & ~here)(lambda: remote().start())
                pl.when(wanted & here)(lambda: local().start())

    def finish_early():
        lax.fori_loop(quad, strips - 1, lambda w, carry: (finish(w), carry)[1], 0)

    def drain_parts(w, carry):
        def tile(c, carry):
            @pl.when(place(side, c)[2] != member)
            def _():
                part_copy(w, c).wait_send()

            return carry

        lax.fori_loop(0, w + 1, tile, 0)
        return carry

    def drain_tiles(w, carry):
        crossing, valid, sends, keeps = role(w)
        pl.when(sends)(lambda: z_copy(w).wait_send())

        @pl.when(keeps)
        def _():
            for wanted, here, remote, local in final_copies(w):
                pl.when(wanted & ~here)(lambda: remote().wait_send())

        return carry

    @pl.when(is_hub)
    def _():
        row = lax.broadcasted_iota(jnp.int32, (LANE, per * half), 0)
        col = lax.broadcasted_iota(jnp.int32, (LANE, per * half), 1)
        band, within = col // half, col % half
        for k in range(tapers):
            hit = (row == band * W + within - k * W) & (within // W == k)
            sel[k * LANE : (k + 1) * LANE, :] = jnp.where(hit, 1.0, 0.0).astype(jnp.bfloat16)

        def step(h, carry):
            w, i = lax.div(h, subs), lax.rem(h, subs)
            for t in range(m):
                dst = buf.at[w, :, :, pl.ds(pl.multiple_of(i * slab + t * rows, rows), rows), :]
                pltpu.make_async_copy(dst, dst, coef_recv.at[w, i, t]).wait()
            relayout(w, i)

            @pl.when(i == subs - 1)
            def _():
                pl.when(w > 0)(lambda: reduce(w - 1))
                gram(w)

            return carry

        meet()
        lax.fori_loop(0, strips * subs, step, 0)
        lax.fori_loop(0, strips - 1, drain_parts, 0)
        reduce(strips - 1)
        finish(strips - 1)
        drain_parts(strips - 1, 0)
        lax.fori_loop(0, strips, drain_tiles, 0)

    for far, s, i, t in order:
        hub, remote, local = coef_copy(far, s, i, t)
        if far:
            remote().wait_send()
        else:
            pl.when(hub != me)(lambda: remote().wait_send())

    width = out_ref.shape[1]
    here = lax.rem(column, shares)
    per_share = m // shares
    deep = subs * rows
    for s in range(splits):
        for sc in range(splits):
            pltpu.make_async_copy(fland.at[s, sc], fland.at[s, sc], fin_recv.at[s, sc]).wait()
        choice = None
        for j in range(shares):
            pieces = [
                fland[s, sc, :, :, i * slab + t * rows : i * slab + (t + 1) * rows].reshape(deep, rows)
                for t in range(j * per_share, (j + 1) * per_share)
                for sc in range(splits)
                for i in range(subs)
            ]
            value = jnp.concatenate(pieces, axis=1)
            choice = value if choice is None else jnp.where(here == j, value, choice)
        row = lax.broadcasted_iota(jnp.int32, (deep, width), 0) + (me * own + s * deep)
        col = lax.broadcasted_iota(jnp.int32, (deep, width), 1) + column * width
        out_ref[s * deep : (s + 1) * deep, :] = jnp.where(row == col, 0.0, choice) * scale


def body(coeffs):
    parts, tapers, own, bins = coeffs.shape
    n = lax.axis_size("chan")
    groups = lax.axis_size("band")
    full = own * n
    m = n // 4
    hubs = 2 * m
    lanes = bins // hubs
    bands = lanes // W
    depth = parts * tapers * W
    strip = LANE
    strips = full // strip
    splits = strips // 4
    subs = min(SUBS, own // splits // 16)
    rows = own // splits // subs
    slab = strip // subs
    members = groups * m
    shares = groups // 4
    scale = W * tapers / (bins // W * groups)
    dma = pltpu.SemaphoreType.DMA

    def run(*refs):
        kernel(scale, *refs)

    return pl.pallas_call(
        run,
        out_shape=pltpu.VMEM((own, full // groups), jnp.float32),
        in_specs=[pl.BlockSpec(memory_space=pl.ANY)],
        out_specs=pl.BlockSpec(memory_space=pltpu.VMEM),
        scratch_shapes=[
            pltpu.VMEM((strips, parts, tapers, strip, lanes), jnp.bfloat16),
            pltpu.VMEM((tapers * LANE, LANE // W * depth // 2), jnp.bfloat16),
            pltpu.VMEM((bands, full, depth), jnp.bfloat16),
            pltpu.VMEM((bands, strip, depth), jnp.bfloat16),
            pltpu.VMEM((strip, LANE), jnp.float32),
            pltpu.VMEM((bands, full), jnp.float32),
            pltpu.VMEM((strips, strips, strip, strip), jnp.float32),
            pltpu.VMEM((strips, members, strip, strip), jnp.float32),
            pltpu.VMEM((strips, strip, strip), jnp.float32),
            pltpu.VMEM((strips, strip, strip), jnp.float32),
            pltpu.VMEM((strips, strip, strip), jnp.float32),
            pltpu.VMEM((strips, 2, subs, m, rows, strip), jnp.float32),
            pltpu.VMEM((splits, splits, subs, rows, strip), jnp.float32),
            dma((2, splits, subs, m)),
            dma((strips, subs, m)),
            dma((strips, strips)),
            dma((strips,)),
            dma((strips,)),
            dma((strips,)),
            dma((strips, 2, m, shares)),
            dma((splits, splits)),
            pltpu.SemaphoreType.REGULAR,
            pltpu.SemaphoreType.REGULAR,
            pltpu.SemaphoreType.REGULAR,
        ],
        compiler_params=pltpu.CompilerParams(
            collective_id=0, has_side_effects=True, vmem_limit_bytes=56 * 1024 * 1024
        ),
    )(coeffs)


def solution(mesh):
    return jax.shard_map(
        body,
        mesh=mesh,
        in_specs=(P(None, None, "chan", "band"),),
        out_specs=P("chan", "band"),
        check_vma=False,
    )
```

```python
import jax
import jax.numpy as jnp
from jax import lax
from jax.experimental import pallas as pl
from jax.experimental.pallas import tpu as pltpu
from jax.sharding import PartitionSpec as P

W = 16
LANE = 128
SUBS = 2

epsilon = 1e-06

MESH = pl.DeviceIdType.MESH


def quarter(side, z):
    seen = z + side * (3 - 2 * z)
    far = seen // 2
    return far * seen + (1 - far) * (1 - seen)


def group(side, q):
    far = q // 2
    seen = far * q + (1 - far) * (1 - q)
    return seen + side * (3 - 2 * seen)


def kernel(
    scale,
    x_ref,
    out_ref,
    buf,
    sel,
    xb,
    left,
    inv_own,
    inv_col,
    inv_row,
    part,
    land,
    fin,
    fland,
    coef_send,
    coef_recv,
    part_send,
    part_recv,
    fin_send,
    fin_recv,
    ready,
    met,
    go,
):
    n = lax.axis_size("chan")
    groups = lax.axis_size("band")
    me = lax.axis_index("chan")
    column = lax.axis_index("band")
    strips, windows, parts, tapers, strip, unused = buf.shape
    lanes = windows * LANE
    splits = fland.shape[1]
    bands, full, depth = xb.shape
    half = depth // 2
    m = n // 4
    own = full // n
    quad = strips // 2
    shares = groups // 4
    members = groups * m
    per = LANE // W
    deep = strip // m
    subs = part.shape[2]
    slab = strip // subs
    rows = deep // subs

    z = lax.div(me, m)
    lane = lax.rem(me, m)
    side = lax.div(z, 2)
    is_hub = (z == 1) | (z == 2)
    member = lane * groups + column
    mine = quarter(side, lax.div(column, shares)) * splits + lane
    reduces = (lane < splits) & (lax.rem(column, shares) == 0)

    barrier = pltpu.get_barrier_semaphore()
    envoy = m + 1
    is_envoy = me == envoy

    @pl.when(is_hub)
    def _():
        for c in range(1, n):
            pl.semaphore_signal(
                barrier, inc=1, device_id={"chan": lax.rem(me + c, n)}, device_id_type=MESH
            )

    @pl.when(is_envoy)
    def _():
        for g in range(1, groups):
            pl.semaphore_signal(
                barrier,
                inc=1,
                device_id={"band": lax.rem(column + g, groups)},
                device_id_type=MESH,
            )

    pl.semaphore_wait(
        barrier, 2 * m - is_hub.astype(jnp.int32) + is_envoy.astype(jnp.int32) * (groups - 1)
    )

    def coef_copy(far, s, v, i, t):
        to_side = side + far * (1 - 2 * side)
        hub = m + to_side * m + t
        w = quarter(to_side, z) * splits + s
        first = (hub - m) * lanes + v * LANE
        src = x_ref.at[
            :, :, pl.ds(s * deep + i * rows, rows), pl.ds(pl.multiple_of(first, LANE), LANE)
        ]
        dst = buf.at[w, v, :, :, pl.ds(pl.multiple_of(i * slab + lane * rows, rows), rows), :]
        recv = coef_recv.at[w, v, i]

        def remote():
            return pltpu.make_async_remote_copy(
                src_ref=src,
                dst_ref=dst,
                send_sem=coef_send.at[far, t],
                recv_sem=recv,
                device_id={"chan": hub},
                device_id_type=MESH,
            )

        return hub, remote, lambda: pltpu.make_async_copy(src, dst, recv)

    order = [
        (far, s, v, i, t)
        for far in range(2)
        for s in range(splits)
        for v in range(windows)
        for i in range(subs)
        for t in range(m)
    ]
    for far, *chunk in order:
        hub, remote, local = coef_copy(far, *chunk)
        if far:
            remote().start()
        else:
            pl.when(hub != me)(lambda: remote().start())
            pl.when(hub == me)(lambda: local().start())

    @pl.when(~is_hub)
    def _():
        pl.semaphore_signal(ready, inc=1, device_id={"chan": envoy}, device_id_type=MESH)

    def meet():
        @pl.when(is_envoy)
        def _():
            pl.semaphore_wait(ready, n - 2 * m)
            for g in range(1, groups):
                pl.semaphore_signal(
                    met,
                    inc=1,
                    device_id={"band": lax.rem(column + g, groups)},
                    device_id_type=MESH,
                )
            pl.semaphore_wait(met, groups - 1)
            for h in range(2 * m):
                if m + h != envoy:
                    pl.semaphore_signal(go, inc=1, device_id={"chan": m + h}, device_id_type=MESH)

        @pl.when(~is_envoy)
        def _():
            pl.semaphore_wait(go, 1)

    last = strips - 1

    def place(c):
        band = group(side, lax.div(c, splits)) * shares
        at = lax.rem(c, splits)
        return band, m + side * m + at, at * groups + band

    def part_copy(w, c, i):
        band, chan, to = place(c)
        return pltpu.make_async_remote_copy(
            src_ref=part.at[w, c, i],
            dst_ref=land.at[w, lax.rem(member - to + members, members), i],
            send_sem=part_send.at[c],
            recv_sem=part_recv.at[w],
            device_id={"band": band, "chan": chan},
            device_id_type=MESH,
        )

    def final_copies(w):
        for turned in range(2):
            row, col = (mine, w) if turned else (w, mine)
            zr, zc = group(side, lax.div(row, splits)), group(side, lax.div(col, splits))
            sr, sc = lax.rem(row, splits), lax.rem(col, splits)
            for t in range(m):
                for j in range(shares):
                    chan, band = zr * m + t, zc * shares + j
                    src = fin.at[w, turned, pl.ds(t * deep, deep), :]
                    dst = fland.at[side, sr, sc]

                    def remote():
                        return pltpu.make_async_remote_copy(
                            src_ref=src,
                            dst_ref=dst,
                            send_sem=fin_send.at[w, turned, j],
                            recv_sem=fin_recv,
                            device_id={"band": band, "chan": chan},
                            device_id_type=MESH,
                        )

                    def local():
                        return pltpu.make_async_copy(src, dst, fin_recv)

                    here = (chan == me) & (band == column)
                    wanted = (w != mine) if turned else True
                    yield row >= quad, wanted, here, remote, local

    def relayout(w, v, i):
        at = lax.broadcasted_iota(jnp.int32, (slab, LANE), 1)
        power = jnp.ones((slab, LANE), jnp.float32)
        spans = [pl.ds(pl.multiple_of(t * deep + i * rows, rows), rows) for t in range(m)]
        homes = [pl.ds(pl.multiple_of(w * strip + t * deep + i * rows, rows), rows) for t in range(m)]
        chunk = pl.ds(pl.multiple_of(i * slab, slab), slab)
        both = jnp.concatenate(
            [
                jnp.concatenate([buf[w, v, p, k, chunk] for k in range(tapers)], axis=1)
                for p in range(parts)
            ],
            axis=0,
        )
        for d in range(per // 2):
            chosen = sel[:, 2 * d * half : 2 * (d + 1) * half]
            picked = jnp.dot(both, chosen, preferred_element_type=jnp.float32)
            for e in range(2):
                near = 2 * d + e
                b = v * per + near
                re = picked[:slab, e * half : (e + 1) * half]
                im = picked[slab:, e * half : (e + 1) * half]
                sums = jnp.sum(re * re + im * im, axis=1, keepdims=True) + epsilon
                power = jnp.where(at == near, sums, power)
                left[near, :slab, :half] = re.astype(jnp.bfloat16)
                left[near, :slab, half:] = im.astype(jnp.bfloat16)
                left[near, slab:, :half] = im.astype(jnp.bfloat16)
                left[near, slab:, half:] = (-re).astype(jnp.bfloat16)
                for t in range(m):
                    segment = slice(t * rows, (t + 1) * rows)
                    xb[b, homes[t], :half] = re[segment].astype(jnp.bfloat16)
                    xb[b, homes[t], half:] = im[segment].astype(jnp.bfloat16)
        inverse = 1.0 / power
        inv_own[...] = inverse
        for t in range(m):
            inv_col[spans[t], :] = inverse[t * rows : (t + 1) * rows]
        inv_row[
            pl.ds(pl.multiple_of(v * per, per), per), pl.ds(pl.multiple_of(w * strip, strip), strip)
        ] = inv_col[...].T[:per, :]

    contract = (((1,), (1,)), ((), ()))

    def gram(w, v, i):
        at = lax.div(column, shares)

        def pair(k, carry):
            seat = jnp.where(
                k == 0,
                3 - at,
                jnp.where(k == 1, lax.rem(at + 2, 4), jnp.where(k == 2, at + 1 - 2 * lax.rem(at, 2), at)),
            )
            u = quarter(side, seat)

            @pl.when(2 * u <= w)
            def _():
                cols = pl.ds(pl.multiple_of(u * 2 * strip, 2 * strip), 2 * strip)
                scales = inv_row[pl.ds(pl.multiple_of(v * per, per), per), cols]
                acc = jnp.zeros((slab, 2 * strip), jnp.float32)
                for d in range(per):
                    b = v * per + d
                    both = lax.dot_general(
                        left[d], xb[b, cols, :], contract, preferred_element_type=jnp.float32
                    )
                    re, im = both[:slab], both[slab:]
                    acc += ((re * re + im * im) * inv_own[:, d : d + 1]) * scales[d : d + 1, :]

                for e in range(2):
                    c = 2 * u + e
                    here = acc[:, e * strip : (e + 1) * strip]
                    if windows == 1:
                        part[w, c, i] = here
                    else:

                        @pl.when(v == 0)
                        def _():
                            part[w, c, i] = here

                        @pl.when(v > 0)
                        def _():
                            part[w, c, i] += here

                for e in range(2):
                    c = 2 * u + e
                    to = place(c)[2]
                    pl.when((v == windows - 1) & (c <= w) & (to != member))(
                        lambda: part_copy(w, c, i).start()
                    )

            return carry

        lax.fori_loop(0, 4, pair, 0)

    def reduce(w):
        @pl.when(reduces & (mine <= w))
        def _():
            every = land.at[w, pl.ds(1, members - 1)]
            pltpu.make_async_copy(every, every, part_recv.at[w]).wait()
            for i in range(subs):
                summed = part[w, mine, i]
                for rel in range(1, members):
                    summed += land[w, rel, i]
                for t in range(m):
                    home = slice(t * deep + i * rows, t * deep + (i + 1) * rows)
                    fin[w, 0, home, :] = summed[t * rows : (t + 1) * rows]
            whole = fin[w, 0]
            turned = whole.T
            fin[w, 1] = turned

            @pl.when(w == mine)
            def _():
                row = lax.broadcasted_iota(jnp.int32, (strip, strip), 0) % deep // rows
                col = lax.broadcasted_iota(jnp.int32, (strip, strip), 1) % deep // rows
                fin[w, 0] = jnp.where(row < col, turned, whole)

            for crossing, wanted, here, remote, local in final_copies(w):
                now = wanted & (~crossing | (w == last))
                pl.when(now & ~here)(lambda: remote().start())
                pl.when(now & here)(lambda: local().start())

    def send_held(w, carry):
        @pl.when(reduces & (mine <= w))
        def _():
            for crossing, wanted, here, remote, local in final_copies(w):
                pl.when(wanted & crossing)(lambda: remote().start())

        return carry

    def drain_parts():
        for c in range(strips):

            @pl.when(place(c)[2] != member)
            def _():
                sent = part.at[pl.ds(c, strips - c), c]
                pltpu.make_async_copy(sent, sent, part_send.at[c]).wait()

    def drain_tiles(w, carry):
        @pl.when(reduces & (mine <= w))
        def _():
            for turned in range(2):
                row, col = (mine, w) if turned else (w, mine)
                ours = group(side, lax.div(row, splits)) == z
                for j in range(shares):
                    band = group(side, lax.div(col, splits)) * shares + j
                    here = ours & (band == column)
                    wanted = (w != mine) if turned else True
                    every = fin.at[w, turned]
                    others = fin.at[w, turned, pl.ds(0, strip - deep), :]
                    sem = fin_send.at[w, turned, j]
                    pl.when(wanted & ~here)(lambda: pltpu.make_async_copy(every, every, sem).wait())
                    pl.when(wanted & here)(lambda: pltpu.make_async_copy(others, others, sem).wait())

        return carry

    @pl.when(is_hub)
    def _():
        row = lax.broadcasted_iota(jnp.int32, (LANE, per * half), 0)
        col = lax.broadcasted_iota(jnp.int32, (LANE, per * half), 1)
        band, within = col // half, col % half
        for k in range(tapers):
            hit = (row == band * W + within - k * W) & (within // W == k)
            sel[k * LANE : (k + 1) * LANE, :] = jnp.where(hit, 1.0, 0.0).astype(jnp.bfloat16)

        def step(h, carry):
            w = lax.div(h, windows * subs)
            v = lax.rem(lax.div(h, subs), windows)
            i = lax.rem(h, subs)
            pl.when((w > 0) & (v == windows - 1) & (i == 0))(lambda: reduce(w - 1))
            dst = buf.at[w, v, :, :, pl.ds(pl.multiple_of(i * slab, slab), slab), :]
            pltpu.make_async_copy(dst, dst, coef_recv.at[w, v, i]).wait()
            relayout(w, v, i)
            gram(w, v, i)
            return carry

        meet()
        lax.fori_loop(0, strips * windows * subs, step, 0)
        lax.fori_loop(quad, last, send_held, 0)
        reduce(last)
        drain_parts()
        lax.fori_loop(0, strips, drain_tiles, 0)

    for far in range(2):
        for t in range(m):
            hub = m + (side + far * (1 - 2 * side)) * m + t
            sent = x_ref.at[:, :, :, pl.ds(pl.multiple_of((hub - m) * lanes, LANE), lanes)]

            @pl.when(hub != me)
            def _():
                pltpu.make_async_copy(sent, sent, coef_send.at[far, t]).wait()

    width = out_ref.shape[1]
    here = lax.rem(column, shares)
    per_share = m // shares
    pltpu.make_async_copy(fland, fland, fin_recv).wait()
    for s in range(splits):
        choice = None
        for j in range(shares):
            pieces = [
                fland[0, s, sc, :, t * deep : (t + 1) * deep]
                + fland[1, s, sc, :, t * deep : (t + 1) * deep]
                for t in range(j * per_share, (j + 1) * per_share)
                for sc in range(splits)
            ]
            value = jnp.concatenate(pieces, axis=1)
            choice = value if choice is None else jnp.where(here == j, value, choice)
        row = lax.broadcasted_iota(jnp.int32, (deep, width), 0) + (me * own + s * deep)
        col = lax.broadcasted_iota(jnp.int32, (deep, width), 1) + column * width
        out_ref[s * deep : (s + 1) * deep, :] = jnp.where(row == col, 0.0, choice) * scale


def body(coeffs):
    parts, tapers, own, bins = coeffs.shape
    n = lax.axis_size("chan")
    groups = lax.axis_size("band")
    full = own * n
    m = n // 4
    hubs = 2 * m
    lanes = bins // hubs
    bands = lanes // W
    depth = parts * tapers * W
    strip = LANE
    strips = full // strip
    splits = strips // 4
    windows = lanes // LANE
    subs = SUBS
    slab = strip // subs
    members = groups * m
    shares = groups // 4
    scale = W * tapers / (bins // W * groups)
    dma = pltpu.SemaphoreType.DMA

    def run(*refs):
        kernel(scale, *refs)

    return pl.pallas_call(
        run,
        out_shape=pltpu.VMEM((own, full // groups), jnp.float32),
        in_specs=[pl.BlockSpec(memory_space=pl.ANY)],
        out_specs=pl.BlockSpec(memory_space=pltpu.VMEM),
        scratch_shapes=[
            pltpu.VMEM((strips, windows, parts, tapers, strip, LANE), jnp.bfloat16),
            pltpu.VMEM((tapers * LANE, LANE // W * depth // 2), jnp.bfloat16),
            pltpu.VMEM((bands, full, depth), jnp.bfloat16),
            pltpu.VMEM((LANE // W, 2 * slab, depth), jnp.bfloat16),
            pltpu.VMEM((slab, LANE), jnp.float32),
            pltpu.VMEM((strip, LANE), jnp.float32),
            pltpu.VMEM((bands, full), jnp.float32),
            pltpu.VMEM((strips, strips, subs, slab, strip), jnp.float32),
            pltpu.VMEM((strips, members, subs, slab, strip), jnp.float32),
            pltpu.VMEM((strips, 2, strip, strip), jnp.float32),
            pltpu.VMEM((2, splits, splits, strip // m, strip), jnp.float32),
            dma((2, m)),
            dma((strips, windows, subs)),
            dma((strips,)),
            dma((strips,)),
            dma((strips, 2, shares)),
            dma,
            pltpu.SemaphoreType.REGULAR,
            pltpu.SemaphoreType.REGULAR,
            pltpu.SemaphoreType.REGULAR,
        ],
        compiler_params=pltpu.CompilerParams(
            collective_id=0, has_side_effects=True, vmem_limit_bytes=56 * 1024 * 1024
        ),
    )(coeffs)


def solution(mesh):
    return jax.shard_map(
        body,
        mesh=mesh,
        in_specs=(P(None, None, "chan", "band"),),
        out_specs=P("chan", "band"),
        check_vma=False,
    )
```

```python
import jax
import jax.numpy as jnp
from jax import lax
from jax.experimental import pallas as pl
from jax.experimental.pallas import tpu as pltpu
from jax.sharding import PartitionSpec as P

W = 16
LANE = 128
SUBS = 2

epsilon = 1e-06

MESH = pl.DeviceIdType.MESH


def quarter(side, z):
    seen = z + side * (3 - 2 * z)
    far = seen // 2
    return far * seen + (1 - far) * (1 - seen)


def group(side, q):
    far = q // 2
    seen = far * q + (1 - far) * (1 - q)
    return seen + side * (3 - 2 * seen)


def kernel(
    scale,
    x_ref,
    out_ref,
    buf,
    sel,
    xb,
    left,
    inv_own,
    inv_col,
    inv_row,
    part,
    land,
    fin,
    fland,
    coef_send,
    coef_recv,
    part_send,
    part_recv,
    fin_send,
    fin_recv,
    ready,
    met,
    go,
):
    n = lax.axis_size("chan")
    groups = lax.axis_size("band")
    me = lax.axis_index("chan")
    column = lax.axis_index("band")
    strips, windows, parts, tapers, strip, unused = buf.shape
    lanes = windows * LANE
    splits = fland.shape[1]
    bands, full, depth = xb.shape
    half = depth // 2
    m = n // 4
    own = full // n
    quad = strips // 2
    shares = groups // 4
    members = groups * m
    per = LANE // W
    deep = strip // m
    subs = part.shape[2]
    slab = strip // subs
    rows = deep // subs

    z = lax.div(me, m)
    lane = lax.rem(me, m)
    side = lax.div(z, 2)
    is_hub = (z == 1) | (z == 2)
    member = lane * groups + column
    mine = quarter(side, lax.div(column, shares)) * splits + lane
    reduces = (lane < splits) & (lax.rem(column, shares) == 0)

    barrier = pltpu.get_barrier_semaphore()
    envoy = m + 1
    is_envoy = me == envoy

    @pl.when(is_hub)
    def _():
        for c in range(1, n):
            pl.semaphore_signal(
                barrier, inc=1, device_id={"chan": lax.rem(me + c, n)}, device_id_type=MESH
            )

    @pl.when(is_envoy)
    def _():
        for g in range(1, groups):
            pl.semaphore_signal(
                barrier,
                inc=1,
                device_id={"band": lax.rem(column + g, groups)},
                device_id_type=MESH,
            )

    pl.semaphore_wait(
        barrier, 2 * m - is_hub.astype(jnp.int32) + is_envoy.astype(jnp.int32) * (groups - 1)
    )

    def coef_copy(far, s, v, i, t):
        to_side = side + far * (1 - 2 * side)
        hub = m + to_side * m + t
        w = quarter(to_side, z) * splits + s
        first = (hub - m) * lanes + v * LANE
        src = x_ref.at[
            :, :, pl.ds(s * deep + i * rows, rows), pl.ds(pl.multiple_of(first, LANE), LANE)
        ]
        dst = buf.at[w, v, :, :, pl.ds(pl.multiple_of(i * slab + lane * rows, rows), rows), :]
        recv = coef_recv.at[w, v, i]

        def remote():
            return pltpu.make_async_remote_copy(
                src_ref=src,
                dst_ref=dst,
                send_sem=coef_send.at[far, t],
                recv_sem=recv,
                device_id={"chan": hub},
                device_id_type=MESH,
            )

        return hub, remote, lambda: pltpu.make_async_copy(src, dst, recv)

    order = [
        (far, s, v, i, t)
        for far in range(2)
        for s in range(splits)
        for v in range(windows)
        for i in range(subs)
        for t in range(m)
    ]
    for far, *chunk in order:
        hub, remote, local = coef_copy(far, *chunk)
        if far:
            remote().start()
        else:
            pl.when(hub != me)(lambda: remote().start())
            pl.when(hub == me)(lambda: local().start())

    @pl.when(~is_hub)
    def _():
        pl.semaphore_signal(ready, inc=1, device_id={"chan": envoy}, device_id_type=MESH)

    def meet():
        @pl.when(is_envoy)
        def _():
            pl.semaphore_wait(ready, n - 2 * m)
            for g in range(1, groups):
                pl.semaphore_signal(
                    met,
                    inc=1,
                    device_id={"band": lax.rem(column + g, groups)},
                    device_id_type=MESH,
                )
            pl.semaphore_wait(met, groups - 1)
            for h in range(2 * m):
                if m + h != envoy:
                    pl.semaphore_signal(go, inc=1, device_id={"chan": m + h}, device_id_type=MESH)

        @pl.when(~is_envoy)
        def _():
            pl.semaphore_wait(go, 1)

    last = strips - 1

    def place(c):
        band = group(side, lax.div(c, splits)) * shares
        at = lax.rem(c, splits)
        return band, m + side * m + at, at * groups + band

    def part_copy(w, c, i):
        band, chan, to = place(c)
        return pltpu.make_async_remote_copy(
            src_ref=part.at[w, c, i],
            dst_ref=land.at[w, lax.rem(member - to + members, members), i],
            send_sem=part_send.at[c],
            recv_sem=part_recv.at[w],
            device_id={"band": band, "chan": chan},
            device_id_type=MESH,
        )

    def final_copies(w):
        for turned in range(2):
            row, col = (mine, w) if turned else (w, mine)
            zr, zc = group(side, lax.div(row, splits)), group(side, lax.div(col, splits))
            sr, sc = lax.rem(row, splits), lax.rem(col, splits)
            for t in range(m):
                for j in range(shares):
                    chan, band = zr * m + t, zc * shares + j
                    src = fin.at[w, turned, pl.ds(t * deep, deep), :]
                    dst = fland.at[side, sr, sc]

                    def remote():
                        return pltpu.make_async_remote_copy(
                            src_ref=src,
                            dst_ref=dst,
                            send_sem=fin_send.at[w, turned, j],
                            recv_sem=fin_recv,
                            device_id={"band": band, "chan": chan},
                            device_id_type=MESH,
                        )

                    def local():
                        return pltpu.make_async_copy(src, dst, fin_recv)

                    here = (chan == me) & (band == column)
                    wanted = (w != mine) if turned else True
                    yield row >= quad, wanted, here, remote, local

    def relayout(w, v, i):
        at = lax.broadcasted_iota(jnp.int32, (slab, LANE), 1)
        power = jnp.ones((slab, LANE), jnp.float32)
        spans = [pl.ds(pl.multiple_of(t * deep + i * rows, rows), rows) for t in range(m)]
        homes = [pl.ds(pl.multiple_of(w * strip + t * deep + i * rows, rows), rows) for t in range(m)]
        chunk = pl.ds(pl.multiple_of(i * slab, slab), slab)
        both = jnp.concatenate(
            [
                jnp.concatenate([buf[w, v, p, k, chunk] for k in range(tapers)], axis=1)
                for p in range(parts)
            ],
            axis=0,
        )
        for d in range(per // 2):
            chosen = sel[:, 2 * d * half : 2 * (d + 1) * half]
            picked = jnp.dot(both, chosen, preferred_element_type=jnp.float32)
            for e in range(2):
                near = 2 * d + e
                b = v * per + near
                re = picked[:slab, e * half : (e + 1) * half]
                im = picked[slab:, e * half : (e + 1) * half]
                sums = jnp.sum(re * re + im * im, axis=1, keepdims=True) + epsilon
                power = jnp.where(at == near, sums, power)
                left[near, :slab, :half] = re.astype(jnp.bfloat16)
                left[near, :slab, half:] = im.astype(jnp.bfloat16)
                left[near, slab:, :half] = im.astype(jnp.bfloat16)
                left[near, slab:, half:] = (-re).astype(jnp.bfloat16)
                for t in range(m):
                    segment = slice(t * rows, (t + 1) * rows)
                    xb[b, homes[t], :half] = re[segment].astype(jnp.bfloat16)
                    xb[b, homes[t], half:] = im[segment].astype(jnp.bfloat16)
        inverse = 1.0 / power
        inv_own[...] = inverse
        for t in range(m):
            inv_col[spans[t], :] = inverse[t * rows : (t + 1) * rows]
        inv_row[
            pl.ds(pl.multiple_of(v * per, per), per), pl.ds(pl.multiple_of(w * strip, strip), strip)
        ] = inv_col[...].T[:per, :]

    contract = (((1,), (1,)), ((), ()))

    def gram(w, v, i):
        at = lax.div(column, shares)

        def pair(k, carry):
            seat = jnp.where(
                k == 0,
                3 - at,
                jnp.where(k == 1, lax.rem(at + 2, 4), jnp.where(k == 2, at + 1 - 2 * lax.rem(at, 2), at)),
            )
            u = quarter(side, seat)

            @pl.when(2 * u <= w)
            def _():
                cols = pl.ds(pl.multiple_of(u * 2 * strip, 2 * strip), 2 * strip)
                scales = inv_row[pl.ds(pl.multiple_of(v * per, per), per), cols]
                acc = jnp.zeros((slab, 2 * strip), jnp.float32)
                for d in range(per):
                    b = v * per + d
                    both = lax.dot_general(
                        left[d], xb[b, cols, :], contract, preferred_element_type=jnp.float32
                    )
                    re, im = both[:slab], both[slab:]
                    acc += ((re * re + im * im) * inv_own[:, d : d + 1]) * scales[d : d + 1, :]

                for e in range(2):
                    c = 2 * u + e
                    here = acc[:, e * strip : (e + 1) * strip]
                    if windows == 1:
                        part[w, c, i] = here
                    else:

                        @pl.when(v == 0)
                        def _():
                            part[w, c, i] = here

                        @pl.when(v > 0)
                        def _():
                            part[w, c, i] += here

                for e in range(2):
                    c = 2 * u + e
                    to = place(c)[2]
                    pl.when((v == windows - 1) & (c <= w) & (to != member))(
                        lambda: part_copy(w, c, i).start()
                    )

            return carry

        lax.fori_loop(0, 4, pair, 0)

    def reduce(w):
        @pl.when(reduces & (mine <= w))
        def _():
            every = land.at[w, pl.ds(1, members - 1)]
            pltpu.make_async_copy(every, every, part_recv.at[w]).wait()
            for i in range(subs):
                summed = part[w, mine, i]
                for rel in range(1, members):
                    summed += land[w, rel, i]
                for t in range(m):
                    home = slice(t * deep + i * rows, t * deep + (i + 1) * rows)
                    fin[w, 0, home, :] = summed[t * rows : (t + 1) * rows]
            whole = fin[w, 0]
            turned = whole.T
            fin[w, 1] = turned

            @pl.when(w == mine)
            def _():
                row = lax.broadcasted_iota(jnp.int32, (strip, strip), 0) % deep // rows
                col = lax.broadcasted_iota(jnp.int32, (strip, strip), 1) % deep // rows
                fin[w, 0] = jnp.where(row < col, turned, whole)

            for crossing, wanted, here, remote, local in final_copies(w):
                now = wanted & (~crossing | (w == last))
                pl.when(now & ~here)(lambda: remote().start())
                pl.when(now & here)(lambda: local().start())

    def send_held(w, carry):
        @pl.when(reduces & (mine <= w))
        def _():
            for crossing, wanted, here, remote, local in final_copies(w):
                pl.when(wanted & crossing)(lambda: remote().start())

        return carry

    def drain_parts():
        for c in range(strips):

            @pl.when(place(c)[2] != member)
            def _():
                sent = part.at[pl.ds(c, strips - c), c]
                pltpu.make_async_copy(sent, sent, part_send.at[c]).wait()

    def drain_tiles(w, carry):
        @pl.when(reduces & (mine <= w))
        def _():
            for turned in range(2):
                row, col = (mine, w) if turned else (w, mine)
                ours = group(side, lax.div(row, splits)) == z
                for j in range(shares):
                    band = group(side, lax.div(col, splits)) * shares + j
                    here = ours & (band == column)
                    wanted = (w != mine) if turned else True
                    every = fin.at[w, turned]
                    others = fin.at[w, turned, pl.ds(0, strip - deep), :]
                    sem = fin_send.at[w, turned, j]
                    pl.when(wanted & ~here)(lambda: pltpu.make_async_copy(every, every, sem).wait())
                    pl.when(wanted & here)(lambda: pltpu.make_async_copy(others, others, sem).wait())

        return carry

    @pl.when(is_hub)
    def _():
        row = lax.broadcasted_iota(jnp.int32, (LANE, per * half), 0)
        col = lax.broadcasted_iota(jnp.int32, (LANE, per * half), 1)
        band, within = col // half, col % half
        for k in range(tapers):
            hit = (row == band * W + within - k * W) & (within // W == k)
            sel[k * LANE : (k + 1) * LANE, :] = jnp.where(hit, 1.0, 0.0).astype(jnp.bfloat16)

        steps = strips * windows * subs

        def step(h, carry):
            w = lax.div(h, windows * subs)
            v = lax.rem(lax.div(h, subs), windows)
            i = lax.rem(h, subs)
            pl.when((w > 0) & (v == windows - 1) & (i == 0))(lambda: reduce(w - 1))
            dst = buf.at[w, v, :, :, pl.ds(pl.multiple_of(i * slab, slab), slab), :]
            pltpu.make_async_copy(dst, dst, coef_recv.at[w, v, i]).wait()

            @pl.when(h == steps - 1)
            def _():
                lax.fori_loop(quad, last, send_held, 0)

            relayout(w, v, i)
            gram(w, v, i)
            return carry

        meet()
        lax.fori_loop(0, steps, step, 0)
        reduce(last)
        drain_parts()
        lax.fori_loop(0, strips, drain_tiles, 0)

    for far in range(2):
        for t in range(m):
            hub = m + (side + far * (1 - 2 * side)) * m + t
            sent = x_ref.at[:, :, :, pl.ds(pl.multiple_of((hub - m) * lanes, LANE), lanes)]

            @pl.when(hub != me)
            def _():
                pltpu.make_async_copy(sent, sent, coef_send.at[far, t]).wait()

    width = out_ref.shape[1]
    here = lax.rem(column, shares)
    per_share = m // shares
    pltpu.make_async_copy(fland, fland, fin_recv).wait()
    for s in range(splits):
        choice = None
        for j in range(shares):
            pieces = [
                fland[0, s, sc, :, t * deep : (t + 1) * deep]
                + fland[1, s, sc, :, t * deep : (t + 1) * deep]
                for t in range(j * per_share, (j + 1) * per_share)
                for sc in range(splits)
            ]
            value = jnp.concatenate(pieces, axis=1)
            choice = value if choice is None else jnp.where(here == j, value, choice)
        row = lax.broadcasted_iota(jnp.int32, (deep, width), 0) + (me * own + s * deep)
        col = lax.broadcasted_iota(jnp.int32, (deep, width), 1) + column * width
        out_ref[s * deep : (s + 1) * deep, :] = jnp.where(row == col, 0.0, choice) * scale


def body(coeffs):
    parts, tapers, own, bins = coeffs.shape
    n = lax.axis_size("chan")
    groups = lax.axis_size("band")
    full = own * n
    m = n // 4
    hubs = 2 * m
    lanes = bins // hubs
    bands = lanes // W
    depth = parts * tapers * W
    strip = LANE
    strips = full // strip
    splits = strips // 4
    windows = lanes // LANE
    subs = SUBS
    slab = strip // subs
    members = groups * m
    shares = groups // 4
    scale = W * tapers / (bins // W * groups)
    dma = pltpu.SemaphoreType.DMA

    def run(*refs):
        kernel(scale, *refs)

    return pl.pallas_call(
        run,
        out_shape=pltpu.VMEM((own, full // groups), jnp.float32),
        in_specs=[pl.BlockSpec(memory_space=pl.ANY)],
        out_specs=pl.BlockSpec(memory_space=pltpu.VMEM),
        scratch_shapes=[
            pltpu.VMEM((strips, windows, parts, tapers, strip, LANE), jnp.bfloat16),
            pltpu.VMEM((tapers * LANE, LANE // W * depth // 2), jnp.bfloat16),
            pltpu.VMEM((bands, full, depth), jnp.bfloat16),
            pltpu.VMEM((LANE // W, 2 * slab, depth), jnp.bfloat16),
            pltpu.VMEM((slab, LANE), jnp.float32),
            pltpu.VMEM((strip, LANE), jnp.float32),
            pltpu.VMEM((bands, full), jnp.float32),
            pltpu.VMEM((strips, strips, subs, slab, strip), jnp.float32),
            pltpu.VMEM((strips, members, subs, slab, strip), jnp.float32),
            pltpu.VMEM((strips, 2, strip, strip), jnp.float32),
            pltpu.VMEM((2, splits, splits, strip // m, strip), jnp.float32),
            dma((2, m)),
            dma((strips, windows, subs)),
            dma((strips,)),
            dma((strips,)),
            dma((strips, 2, shares)),
            dma,
            pltpu.SemaphoreType.REGULAR,
            pltpu.SemaphoreType.REGULAR,
            pltpu.SemaphoreType.REGULAR,
        ],
        compiler_params=pltpu.CompilerParams(
            collective_id=0, has_side_effects=True, vmem_limit_bytes=56 * 1024 * 1024
        ),
    )(coeffs)


def solution(mesh):
    return jax.shard_map(
        body,
        mesh=mesh,
        in_specs=(P(None, None, "chan", "band"),),
        out_specs=P("chan", "band"),
        check_vma=False,
    )
```

```python
import jax
import jax.numpy as jnp
from jax import lax
from jax.experimental import pallas as pl
from jax.experimental.pallas import tpu as pltpu
from jax.sharding import PartitionSpec as P

W = 16
LANE = 128
SUBS = 2

epsilon = 1e-06

MESH = pl.DeviceIdType.MESH


def quarter(side, z):
    seen = z + side * (3 - 2 * z)
    far = seen // 2
    return far * seen + (1 - far) * (1 - seen)


def group(side, q):
    far = q // 2
    seen = far * q + (1 - far) * (1 - q)
    return seen + side * (3 - 2 * seen)


def kernel(
    scale,
    x_ref,
    out_ref,
    buf,
    sel,
    xb,
    left,
    inv_own,
    inv_col,
    inv_row,
    part,
    land,
    fin,
    fland,
    coef_send,
    coef_recv,
    part_send,
    part_recv,
    fin_send,
    fin_recv,
    ready,
    met,
    go,
):
    n = lax.axis_size("chan")
    groups = lax.axis_size("band")
    me = lax.axis_index("chan")
    column = lax.axis_index("band")
    strips, windows, parts, tapers, strip, unused = buf.shape
    lanes = windows * LANE
    splits = fland.shape[1]
    bands, full, depth = xb.shape
    half = depth // 2
    m = n // 4
    own = full // n
    quad = strips // 2
    shares = groups // 4
    members = groups * m
    per = LANE // W
    deep = strip // m
    subs = part.shape[2]
    slab = strip // subs
    rows = deep // subs

    z = lax.div(me, m)
    lane = lax.rem(me, m)
    side = lax.div(z, 2)
    is_hub = (z == 1) | (z == 2)
    member = lane * groups + column
    mine = quarter(side, lax.div(column, shares)) * splits + lane
    reduces = (lane < splits) & (lax.rem(column, shares) == 0)

    barrier = pltpu.get_barrier_semaphore()
    envoy = m + 1
    is_envoy = me == envoy

    @pl.when(is_hub)
    def _():
        for c in range(1, n):
            pl.semaphore_signal(
                barrier, inc=1, device_id={"chan": lax.rem(me + c, n)}, device_id_type=MESH
            )

    @pl.when(is_envoy)
    def _():
        for g in range(1, groups):
            pl.semaphore_signal(
                barrier,
                inc=1,
                device_id={"band": lax.rem(column + g, groups)},
                device_id_type=MESH,
            )

    pl.semaphore_wait(
        barrier, 2 * m - is_hub.astype(jnp.int32) + is_envoy.astype(jnp.int32) * (groups - 1)
    )

    def coef_copy(far, s, v, i, t):
        to_side = side + far * (1 - 2 * side)
        hub = m + to_side * m + t
        w = quarter(to_side, z) * splits + s
        first = (hub - m) * lanes + v * LANE
        src = x_ref.at[
            :, :, pl.ds(s * deep + i * rows, rows), pl.ds(pl.multiple_of(first, LANE), LANE)
        ]
        dst = buf.at[w, v, :, :, pl.ds(pl.multiple_of(i * slab + lane * rows, rows), rows), :]
        recv = coef_recv.at[w, v, i]

        def remote():
            return pltpu.make_async_remote_copy(
                src_ref=src,
                dst_ref=dst,
                send_sem=coef_send.at[far, t],
                recv_sem=recv,
                device_id={"chan": hub},
                device_id_type=MESH,
            )

        return hub, remote, lambda: pltpu.make_async_copy(src, dst, recv)

    order = [
        (far, s, v, i, t)
        for far in range(2)
        for s in range(splits)
        for v in range(windows)
        for i in range(subs)
        for t in range(m)
    ]
    for far, *chunk in order:
        hub, remote, local = coef_copy(far, *chunk)
        if far:
            remote().start()
        else:
            pl.when(hub != me)(lambda: remote().start())
            pl.when(hub == me)(lambda: local().start())

    @pl.when(~is_hub)
    def _():
        pl.semaphore_signal(ready, inc=1, device_id={"chan": envoy}, device_id_type=MESH)

    def meet():
        @pl.when(is_envoy)
        def _():
            pl.semaphore_wait(ready, n - 2 * m)
            for g in range(1, groups):
                pl.semaphore_signal(
                    met,
                    inc=1,
                    device_id={"band": lax.rem(column + g, groups)},
                    device_id_type=MESH,
                )
            pl.semaphore_wait(met, groups - 1)
            for h in range(2 * m):
                if m + h != envoy:
                    pl.semaphore_signal(go, inc=1, device_id={"chan": m + h}, device_id_type=MESH)

        @pl.when(~is_envoy)
        def _():
            pl.semaphore_wait(go, 1)

    last = strips - 1

    def place(c):
        band = group(side, lax.div(c, splits)) * shares
        at = lax.rem(c, splits)
        return band, m + side * m + at, at * groups + band

    def part_copy(w, c, i):
        band, chan, to = place(c)
        return pltpu.make_async_remote_copy(
            src_ref=part.at[w, c, i],
            dst_ref=land.at[w, lax.rem(member - to + members, members), i],
            send_sem=part_send.at[c],
            recv_sem=part_recv.at[w],
            device_id={"band": band, "chan": chan},
            device_id_type=MESH,
        )

    def final_copies(w):
        for turned in range(2):
            row, col = (mine, w) if turned else (w, mine)
            zr, zc = group(side, lax.div(row, splits)), group(side, lax.div(col, splits))
            sr, sc = lax.rem(row, splits), lax.rem(col, splits)
            for t in range(m):
                for j in range(shares):
                    chan, band = zr * m + t, zc * shares + j
                    src = fin.at[w, turned, pl.ds(t * deep, deep), :]
                    dst = fland.at[side, sr, sc]

                    def remote():
                        return pltpu.make_async_remote_copy(
                            src_ref=src,
                            dst_ref=dst,
                            send_sem=fin_send.at[w, turned, j],
                            recv_sem=fin_recv,
                            device_id={"band": band, "chan": chan},
                            device_id_type=MESH,
                        )

                    def local():
                        return pltpu.make_async_copy(src, dst, fin_recv)

                    here = (chan == me) & (band == column)
                    wanted = (w != mine) if turned else True
                    yield row >= quad, wanted, here, remote, local

    def relayout(w, v, i):
        at = lax.broadcasted_iota(jnp.int32, (slab, LANE), 1)
        power = jnp.ones((slab, LANE), jnp.float32)
        spans = [pl.ds(pl.multiple_of(t * deep + i * rows, rows), rows) for t in range(m)]
        homes = [pl.ds(pl.multiple_of(w * strip + t * deep + i * rows, rows), rows) for t in range(m)]
        chunk = pl.ds(pl.multiple_of(i * slab, slab), slab)
        both = jnp.concatenate(
            [
                jnp.concatenate([buf[w, v, p, k, chunk] for k in range(tapers)], axis=1)
                for p in range(parts)
            ],
            axis=0,
        )
        for d in range(per // 2):
            chosen = sel[:, 2 * d * half : 2 * (d + 1) * half]
            picked = jnp.dot(both, chosen, preferred_element_type=jnp.float32)
            for e in range(2):
                near = 2 * d + e
                b = v * per + near
                re = picked[:slab, e * half : (e + 1) * half]
                im = picked[slab:, e * half : (e + 1) * half]
                sums = jnp.sum(re * re + im * im, axis=1, keepdims=True) + epsilon
                power = jnp.where(at == near, sums, power)
                left[near, :slab, :half] = re.astype(jnp.bfloat16)
                left[near, :slab, half:] = im.astype(jnp.bfloat16)
                left[near, slab:, :half] = im.astype(jnp.bfloat16)
                left[near, slab:, half:] = (-re).astype(jnp.bfloat16)
                for t in range(m):
                    segment = slice(t * rows, (t + 1) * rows)
                    xb[b, homes[t], :half] = re[segment].astype(jnp.bfloat16)
                    xb[b, homes[t], half:] = im[segment].astype(jnp.bfloat16)
        inverse = 1.0 / power
        inv_own[...] = inverse
        for t in range(m):
            inv_col[spans[t], :] = inverse[t * rows : (t + 1) * rows]
        inv_row[
            pl.ds(pl.multiple_of(v * per, per), per), pl.ds(pl.multiple_of(w * strip, strip), strip)
        ] = inv_col[...].T[:per, :]

    contract = (((1,), (1,)), ((), ()))

    def gram(w, v, i):
        at = lax.div(column, shares)

        def pair(k, carry):
            seat = jnp.where(
                k == 0,
                at + 1 - 2 * lax.rem(at, 2),
                jnp.where(k == 1, 3 - at, jnp.where(k == 2, lax.rem(at + 2, 4), at)),
            )
            u = quarter(side, seat)

            @pl.when(2 * u <= w)
            def _():
                cols = pl.ds(pl.multiple_of(u * 2 * strip, 2 * strip), 2 * strip)
                scales = inv_row[pl.ds(pl.multiple_of(v * per, per), per), cols]
                acc = jnp.zeros((slab, 2 * strip), jnp.float32)
                for d in range(per):
                    b = v * per + d
                    both = lax.dot_general(
                        left[d], xb[b, cols, :], contract, preferred_element_type=jnp.float32
                    )
                    re, im = both[:slab], both[slab:]
                    acc += ((re * re + im * im) * inv_own[:, d : d + 1]) * scales[d : d + 1, :]

                for e in range(2):
                    c = 2 * u + e
                    here = acc[:, e * strip : (e + 1) * strip]
                    if windows == 1:
                        part[w, c, i] = here
                    else:

                        @pl.when(v == 0)
                        def _():
                            part[w, c, i] = here

                        @pl.when(v > 0)
                        def _():
                            part[w, c, i] += here

                for e in range(2):
                    c = 2 * u + e
                    to = place(c)[2]
                    pl.when((v == windows - 1) & (c <= w) & (to != member))(
                        lambda: part_copy(w, c, i).start()
                    )

            return carry

        lax.fori_loop(0, 4, pair, 0)

    def reduce(w):
        @pl.when(reduces & (mine <= w))
        def _():
            every = land.at[w, pl.ds(1, members - 1)]
            pltpu.make_async_copy(every, every, part_recv.at[w]).wait()
            for i in range(subs):
                summed = part[w, mine, i]
                for rel in range(1, members):
                    summed += land[w, rel, i]
                for t in range(m):
                    home = slice(t * deep + i * rows, t * deep + (i + 1) * rows)
                    fin[w, 0, home, :] = summed[t * rows : (t + 1) * rows]
            whole = fin[w, 0]
            turned = whole.T
            fin[w, 1] = turned

            @pl.when(w == mine)
            def _():
                row = lax.broadcasted_iota(jnp.int32, (strip, strip), 0) % deep // rows
                col = lax.broadcasted_iota(jnp.int32, (strip, strip), 1) % deep // rows
                fin[w, 0] = jnp.where(row < col, turned, whole)

            for crossing, wanted, here, remote, local in final_copies(w):
                now = wanted & (~crossing | (w == last))
                pl.when(now & ~here)(lambda: remote().start())
                pl.when(now & here)(lambda: local().start())

    def send_held(w, carry):
        @pl.when(reduces & (mine <= w))
        def _():
            for crossing, wanted, here, remote, local in final_copies(w):
                pl.when(wanted & crossing)(lambda: remote().start())

        return carry

    def drain_parts():
        for c in range(strips):

            @pl.when(place(c)[2] != member)
            def _():
                sent = part.at[pl.ds(c, strips - c), c]
                pltpu.make_async_copy(sent, sent, part_send.at[c]).wait()

    def drain_tiles(w, carry):
        @pl.when(reduces & (mine <= w))
        def _():
            for turned in range(2):
                row, col = (mine, w) if turned else (w, mine)
                ours = group(side, lax.div(row, splits)) == z
                for j in range(shares):
                    band = group(side, lax.div(col, splits)) * shares + j
                    here = ours & (band == column)
                    wanted = (w != mine) if turned else True
                    every = fin.at[w, turned]
                    others = fin.at[w, turned, pl.ds(0, strip - deep), :]
                    sem = fin_send.at[w, turned, j]
                    pl.when(wanted & ~here)(lambda: pltpu.make_async_copy(every, every, sem).wait())
                    pl.when(wanted & here)(lambda: pltpu.make_async_copy(others, others, sem).wait())

        return carry

    @pl.when(is_hub)
    def _():
        row = lax.broadcasted_iota(jnp.int32, (LANE, per * half), 0)
        col = lax.broadcasted_iota(jnp.int32, (LANE, per * half), 1)
        band, within = col // half, col % half
        for k in range(tapers):
            hit = (row == band * W + within - k * W) & (within // W == k)
            sel[k * LANE : (k + 1) * LANE, :] = jnp.where(hit, 1.0, 0.0).astype(jnp.bfloat16)

        steps = strips * windows * subs

        def step(h, carry):
            w = lax.div(h, windows * subs)
            v = lax.rem(lax.div(h, subs), windows)
            i = lax.rem(h, subs)
            pl.when((w > 0) & (v == windows - 1) & (i == 0))(lambda: reduce(w - 1))
            dst = buf.at[w, v, :, :, pl.ds(pl.multiple_of(i * slab, slab), slab), :]
            pltpu.make_async_copy(dst, dst, coef_recv.at[w, v, i]).wait()

            @pl.when(h == steps - 1)
            def _():
                lax.fori_loop(quad, last, send_held, 0)

            relayout(w, v, i)
            gram(w, v, i)
            return carry

        meet()
        lax.fori_loop(0, steps, step, 0)
        reduce(last)
        drain_parts()
        lax.fori_loop(0, strips, drain_tiles, 0)

    for far in range(2):
        for t in range(m):
            hub = m + (side + far * (1 - 2 * side)) * m + t
            sent = x_ref.at[:, :, :, pl.ds(pl.multiple_of((hub - m) * lanes, LANE), lanes)]

            @pl.when(hub != me)
            def _():
                pltpu.make_async_copy(sent, sent, coef_send.at[far, t]).wait()

    width = out_ref.shape[1]
    here = lax.rem(column, shares)
    per_share = m // shares
    pltpu.make_async_copy(fland, fland, fin_recv).wait()
    for s in range(splits):
        choice = None
        for j in range(shares):
            pieces = [
                fland[0, s, sc, :, t * deep : (t + 1) * deep]
                + fland[1, s, sc, :, t * deep : (t + 1) * deep]
                for t in range(j * per_share, (j + 1) * per_share)
                for sc in range(splits)
            ]
            value = jnp.concatenate(pieces, axis=1)
            choice = value if choice is None else jnp.where(here == j, value, choice)
        row = lax.broadcasted_iota(jnp.int32, (deep, width), 0) + (me * own + s * deep)
        col = lax.broadcasted_iota(jnp.int32, (deep, width), 1) + column * width
        out_ref[s * deep : (s + 1) * deep, :] = jnp.where(row == col, 0.0, choice) * scale


def body(coeffs):
    parts, tapers, own, bins = coeffs.shape
    n = lax.axis_size("chan")
    groups = lax.axis_size("band")
    full = own * n
    m = n // 4
    hubs = 2 * m
    lanes = bins // hubs
    bands = lanes // W
    depth = parts * tapers * W
    strip = LANE
    strips = full // strip
    splits = strips // 4
    windows = lanes // LANE
    subs = SUBS
    slab = strip // subs
    members = groups * m
    shares = groups // 4
    scale = W * tapers / (bins // W * groups)
    dma = pltpu.SemaphoreType.DMA

    def run(*refs):
        kernel(scale, *refs)

    return pl.pallas_call(
        run,
        out_shape=pltpu.VMEM((own, full // groups), jnp.float32),
        in_specs=[pl.BlockSpec(memory_space=pl.ANY)],
        out_specs=pl.BlockSpec(memory_space=pltpu.VMEM),
        scratch_shapes=[
            pltpu.VMEM((strips, windows, parts, tapers, strip, LANE), jnp.bfloat16),
            pltpu.VMEM((tapers * LANE, LANE // W * depth // 2), jnp.bfloat16),
            pltpu.VMEM((bands, full, depth), jnp.bfloat16),
            pltpu.VMEM((LANE // W, 2 * slab, depth), jnp.bfloat16),
            pltpu.VMEM((slab, LANE), jnp.float32),
            pltpu.VMEM((strip, LANE), jnp.float32),
            pltpu.VMEM((bands, full), jnp.float32),
            pltpu.VMEM((strips, strips, subs, slab, strip), jnp.float32),
            pltpu.VMEM((strips, members, subs, slab, strip), jnp.float32),
            pltpu.VMEM((strips, 2, strip, strip), jnp.float32),
            pltpu.VMEM((2, splits, splits, strip // m, strip), jnp.float32),
            dma((2, m)),
            dma((strips, windows, subs)),
            dma((strips,)),
            dma((strips,)),
            dma((strips, 2, shares)),
            dma,
            pltpu.SemaphoreType.REGULAR,
            pltpu.SemaphoreType.REGULAR,
            pltpu.SemaphoreType.REGULAR,
        ],
        compiler_params=pltpu.CompilerParams(
            collective_id=0, has_side_effects=True, vmem_limit_bytes=56 * 1024 * 1024
        ),
    )(coeffs)


def solution(mesh):
    return jax.shard_map(
        body,
        mesh=mesh,
        in_specs=(P(None, None, "chan", "band"),),
        out_specs=P("chan", "band"),
        check_vma=False,
    )
```
